32 devices in a mesh: dom: 8 (over z, x), feat: 4 (over y, core).
Axes of the slice: x: 2, y: 2, z: 4, core: 2. Of those that a mesh axis runs over, the one named last changes fastest.
Arguments:
- grid_feat: bfloat16 [16384, 512], P(('dom', 'feat')), may hold values from -6 to 6
- mesh_feat: bfloat16 [1280, 512], P(('dom', 'feat')), may hold values from -6 to 6
- w_grid: bfloat16 [512, 512], P('feat'), may hold values from -0.25 to 0.25
- w_mesh: bfloat16 [512, 512], P('feat'), may hold values from -0.25 to 0.25
- w_enc2: bfloat16 [512, 512], P('feat'), may hold values from -0.25 to 0.25
- w_src: bfloat16 [512, 512], P('feat'), may hold values from -0.25 to 0.25
- w_dst: bfloat16 [512, 512], P('feat'), may hold values from -0.25 to 0.25
- w_proc2: bfloat16 [512, 512], P('feat'), may hold values from -0.25 to 0.25
- enc_send: int32 [256, 2], P(('dom', 'feat')), may hold values from -1 to 511, as said below
- enc_dst: int32 [256, 2], P(('dom', 'feat')), may hold values from -1 to 159, as said below
- hal_send: int32 [64, 4], P('dom'), may hold values from -1 to 159, as said below
- proc_src: int32 [5120], P(('dom', 'feat')), may hold values from 0 to 191, as said below
- proc_dst: int32 [5120], P(('dom', 'feat')), may hold values from 0 to 159
- cotangent: bfloat16 [1280, 512], P(('dom', 'feat')), may hold values from -6 to 6
Outputs:
- out: bfloat16 [1280, 512], P(('dom', 'feat'))
- g_grid: bfloat16 [16384, 512], P(('dom', 'feat'))
- g_mesh: bfloat16 [1280, 512], P(('dom', 'feat'))
- g_wgrid: float32 [512, 512], P('feat')
- g_wmesh: float32 [512, 512], P('feat')
- g_wenc2: float32 [512, 512], P('feat')
- g_wsrc: float32 [512, 512], P('feat')
- g_wdst: float32 [512, 512], P('feat')
- g_wproc2: float32 [512, 512], P('feat')
The draws below stay inside these ranges and needn't reach their ends.
Inputs may be any that keep to these rules, and one draw needn't show every extreme that they name: `enc_send`: row j * 8 + r lists, for sender device j, the local grid rows of its slots to partition r in the first n slots and -1 after them; enc_dst's row of the receiver (r, f) for that sender partition has the same n live slots. A quarter of the partitions get half or more of the slots from every sender, and one gets all 2 from every sender. `enc_dst`: row (r * 4 + f) * 8 + s gives the target node, within partition r, of each slot that device s * 4 + f sends to device (r, f); -1 exactly where enc_send's slot is -1. `hal_send`: row s * 8 + r lists the rows of partition s sent to partition r; each pair has 1 to 4 live slots first, -1 after them; some pairs are full. `proc_src`: A value under 160 is a node of the edge's own partition; a value 160 + s * 4 + c names halo slot c from partition s, always a live one.
All inputs are finite; a program needn't handle non-finite values.
Results may differ from the reference program's by a relative error of at most 0.014.
Values may be sent and summed in bfloat16 or wider, within the bound.
A program may use at most 64 MiB of HBM per device.

```python
import math
import jax
import jax.numpy as jnp
from jax import lax

D = 512
G_DEV = 512
M_DEV = 40
CAP = 2
HCAP = 4
E_DEV = 160
PART = 160
GRID = 16384
MESH = 1280
EDGES = 5120
N_DOM = 8
N_FEAT = 4


def enc_counts(key):
    base = jax.random.fold_in(key, 101)
    order_key, heavy_key, light_key = jax.random.split(base, 3)
    ranking = jax.random.permutation(order_key, N_DOM)
    quarter = max(N_DOM // 4, 1)
    senders = N_DOM * N_FEAT
    heavy = jax.random.randint(heavy_key, (senders, N_DOM), CAP // 2, CAP + 1)
    light = jax.random.randint(light_key, (senders, N_DOM), 0, CAP // 2 + 1)
    counts = jnp.where((ranking < quarter)[None, :], heavy, light)
    return jnp.where((ranking == 0)[None, :], CAP, counts).astype(jnp.int32)


def halo_counts(key):
    base = jax.random.fold_in(key, 201)
    counts = jax.random.randint(base, (N_DOM, N_DOM), 1, HCAP + 1)
    source = jnp.arange(N_DOM, dtype=jnp.int32)
    paired = source[None, :] == (source[:, None] + 1) % N_DOM
    return jnp.where(paired, HCAP, counts).astype(jnp.int32)


def draw_enc_send(key, part):
    counts = enc_counts(key)
    picks = jax.random.randint(jax.random.fold_in(key, 102), (N_DOM * N_FEAT, N_DOM, CAP), 0, G_DEV)
    column = jnp.arange(CAP, dtype=jnp.int32)
    filled = jnp.where(column[None, None, :] < counts[:, :, None], picks, -1)
    return filled.reshape(N_DOM * N_FEAT * N_DOM, CAP).astype(jnp.int32)


def draw_enc_dst(key, part):
    counts = enc_counts(key).reshape(N_DOM, N_FEAT, N_DOM)
    flipped = jnp.transpose(counts, (2, 1, 0)).reshape(N_DOM * N_FEAT, N_DOM)
    picks = jax.random.randint(jax.random.fold_in(key, 103), (N_DOM * N_FEAT, N_DOM, CAP), 0, M_DEV * N_FEAT)
    column = jnp.arange(CAP, dtype=jnp.int32)
    filled = jnp.where(column[None, None, :] < flipped[:, :, None], picks, -1)
    return filled.reshape(N_DOM * N_FEAT * N_DOM, CAP).astype(jnp.int32)


def draw_hal_send(key, part):
    counts = halo_counts(key)
    picks = jax.random.randint(jax.random.fold_in(key, 202), (N_DOM, N_DOM, HCAP), 0, M_DEV * N_FEAT)
    column = jnp.arange(HCAP, dtype=jnp.int32)
    filled = jnp.where(column[None, None, :] < counts[:, :, None], picks, -1)
    return filled.reshape(N_DOM * N_DOM, HCAP).astype(jnp.int32)


def draw_proc_src(key, part):
    counts = halo_counts(key)
    devices = N_DOM * N_FEAT
    owner = (jnp.arange(devices, dtype=jnp.int32) // N_FEAT)[:, None]
    pick_key, local_key, source_key, spread_key = jax.random.split(jax.random.fold_in(key, 203), 4)
    choose = jax.random.randint(pick_key, (devices, E_DEV), 0, 2)
    local = jax.random.randint(local_key, (devices, E_DEV), 0, M_DEV * N_FEAT)
    source = jax.random.randint(source_key, (devices, E_DEV), 0, N_DOM)
    spread = jax.random.randint(spread_key, (devices, E_DEV), 0, 1 << 20)
    available = counts[source, owner]
    remote = M_DEV * N_FEAT + source * HCAP + spread % available
    return jnp.where(choose == 1, remote, local).reshape(-1).astype(jnp.int32)


def touch_ends(array, rng, least, largest):
    dims = array.shape
    place = [jax.random.randint(jax.random.fold_in(rng, axis), (), 0, dims[axis]) for axis in range(len(dims))]
    array = array.at[tuple(place)].set(least)
    longest = dims.index(max(dims))
    place[longest] = (place[longest] + 1) % dims[longest]
    return array.at[tuple(place)].set(largest)


def block_scale(rng, dims, cuts, low, high):
    loudness, own = 1.0, jax.random.fold_in(rng, 6)
    for dim, blocks in cuts:
        draws = jnp.exp(jax.random.uniform(jax.random.fold_in(own, dim), (blocks,), jnp.float32, low / len(cuts), high / len(cuts)))
        loudness = loudness * jnp.repeat(draws, dims[dim] // blocks).reshape([-1 if axis == dim else 1 for axis in range(len(dims))])
    return loudness


def normal_values(rng, extent, deviation, reach, cuts=(), kind=jnp.bfloat16):
    entries = deviation * jax.random.normal(rng, extent, jnp.float32)
    if cuts:
        entries = entries * block_scale(rng, extent, cuts, -0.22, 0.18)
    return jnp.clip(entries, -reach, reach).astype(kind)


def setup_inputs(seed: int = 0) -> dict:
    keys = jax.random.split(jax.random.key(seed), 15)
    return {
        "grid_feat": normal_values(keys[0], (GRID, D), 1.0, 6.0, ((0, 32),)),
        "mesh_feat": normal_values(keys[1], (MESH, D), 1.0, 6.0, ((0, 32),)),
        "w_grid": normal_values(keys[2], (D, D), D ** -0.5, 0.25, ((0, 4),)),
        "w_mesh": normal_values(keys[3], (D, D), D ** -0.5, 0.25, ((0, 4),)),
        "w_enc2": normal_values(keys[4], (D, D), D ** -0.5, 0.25, ((0, 4),)),
        "w_src": normal_values(keys[5], (D, D), D ** -0.5, 0.25, ((0, 4),)),
        "w_dst": normal_values(keys[6], (D, D), D ** -0.5, 0.25, ((0, 4),)),
        "w_proc2": normal_values(keys[7], (D, D), D ** -0.5, 0.25, ((0, 4),)),
        "enc_send": draw_enc_send(jax.random.fold_in(keys[14], 71), 0),
        "enc_dst": draw_enc_dst(jax.random.fold_in(keys[14], 71), 0),
        "hal_send": draw_hal_send(jax.random.fold_in(keys[14], 71), 0),
        "proc_src": draw_proc_src(jax.random.fold_in(keys[14], 71), 0),
        "proc_dst": touch_ends(jax.random.randint(keys[12], (EDGES,), 0, PART), jax.random.fold_in(keys[12], 1), 0, PART - 1).astype(jnp.int32),
        "cotangent": normal_values(keys[13], (MESH, D), 1.0, 6.0, ((0, 32),)),
    }


EPS = 1e-05

def matmul(left, right):
    return jnp.dot(left, right, preferred_element_type=jnp.float32)

def matmul_t(left, right):
    return lax.dot_general(left, right, (((left.ndim - 1,), (1,)), ((), ())), preferred_element_type=jnp.float32)

def outer_batch(left, right):
    return jnp.einsum('fnd,fne->fde', left.astype(jnp.float32), right.astype(jnp.float32), precision=lax.Precision.HIGHEST)

def layer_norm(values):
    center = values - lax.optimization_barrier(jnp.mean(values, axis=-1, keepdims=True))
    spread = lax.optimization_barrier(jnp.mean(center * center, axis=-1, keepdims=True))
    scaling = lax.rsqrt(spread + EPS)
    return (center * scaling, scaling)

def norm_back(normed, scaling, upstream):
    inner = lax.optimization_barrier(jnp.mean(upstream, axis=-1, keepdims=True))
    along = lax.optimization_barrier(jnp.mean(upstream * normed, axis=-1, keepdims=True))
    return scaling * (upstream - inner - normed * along)

def silu_slope(preact):
    sigma = jax.nn.sigmoid(preact)
    return sigma * (1.0 + preact * (1.0 - sigma))

def edge_forward(preact, weight):
    hidden = jax.nn.silu(preact).astype(jnp.bfloat16)
    normed, scaling = layer_norm(matmul(hidden, weight))
    return (hidden, normed, scaling)

def rounded_sum(pieces):
    narrow = lax.optimization_barrier(pieces.astype(jnp.bfloat16))
    return lax.optimization_barrier(jnp.sum(narrow.astype(jnp.float32), axis=0))

def reference(grid_feat, mesh_feat, w_grid, w_mesh, w_enc2, w_src, w_dst, w_proc2, enc_send, enc_dst, hal_send, proc_src, proc_dst, cotangent):
    device_count = N_DOM * N_FEAT
    part_rows = M_DEV * N_FEAT
    table_rows = part_rows + N_DOM * HCAP
    factor = 1.0 / math.sqrt(M_DEV * device_count)
    feat_ids = jnp.arange(N_FEAT, dtype=jnp.int32)
    dom_ids = jnp.arange(N_DOM, dtype=jnp.int32)
    sender_dev = dom_ids[None, :] * N_FEAT + feat_ids[:, None]
    grid_dev = grid_feat.reshape(device_count, G_DEV, D)
    projected = matmul(grid_feat, w_grid).astype(jnp.bfloat16).reshape(device_count, G_DEV, D)
    send_idx = enc_send.reshape(device_count, N_DOM, CAP)
    dst_all = enc_dst.reshape(N_DOM, N_FEAT, N_DOM * CAP)
    mesh_all = mesh_feat.reshape(N_DOM, part_rows, D)
    zero_square = jnp.zeros((D, D), jnp.float32)

    def encoder_values(dom_index):
        rows_idx = send_idx[sender_dev, dom_index]
        received = projected[sender_dev[:, :, None], jnp.maximum(rows_idx, 0)]
        received = jnp.where((rows_idx >= 0)[..., None], received, jnp.zeros_like(received))
        targets_raw = dst_all[dom_index]
        targets = jnp.maximum(targets_raw, 0)
        valid = (targets_raw >= 0).astype(jnp.float32)[..., None]
        mesh_part = mesh_all[dom_index]
        node_proj = matmul(mesh_part, w_mesh)
        preact = received.reshape(N_FEAT, N_DOM * CAP, D).astype(jnp.float32) + node_proj[targets]
        hidden, normed, scaling = edge_forward(preact, w_enc2)
        return (mesh_part, targets, valid, preact, hidden, normed, scaling)

    def encode(dom_index):
        mesh_part, targets, valid, preact, hidden, normed, scaling = encoder_values(dom_index)
        summed = jax.ops.segment_sum((normed * valid).reshape(-1, D), targets.reshape(-1), num_segments=part_rows)
        return (mesh_part.astype(jnp.float32) + summed).astype(jnp.bfloat16)
    latent = lax.map(encode, dom_ids)
    hal_idx = hal_send.reshape(N_DOM, N_DOM, HCAP)
    src_all = proc_src.reshape(N_DOM, N_FEAT, E_DEV)
    dstp_all = proc_dst.reshape(N_DOM, N_FEAT, E_DEV)
    cot_all = cotangent.reshape(N_DOM, part_rows, D)

    def process(carry, dom_index):
        node_rows = latent[dom_index]
        wanted = hal_idx[:, dom_index, :]
        halo_rows = latent[dom_ids[:, None], jnp.maximum(wanted, 0)]
        halo_rows = jnp.where((wanted >= 0)[..., None], halo_rows, jnp.zeros_like(halo_rows))
        lookup = jnp.concatenate([node_rows, halo_rows.reshape(N_DOM * HCAP, D)], axis=0)
        sources = src_all[dom_index]
        targets = dstp_all[dom_index]
        src_rows = lookup[sources]
        dst_rows = node_rows[targets]
        preact = matmul(src_rows, w_src) + matmul(dst_rows, w_dst)
        hidden, normed, scaling = edge_forward(preact, w_proc2)
        summed = jax.ops.segment_sum(normed.reshape(-1, D), targets.reshape(-1), num_segments=part_rows)
        out_part = (node_rows.astype(jnp.float32) + summed).astype(jnp.bfloat16)
        cot_rows = cot_all[dom_index].astype(jnp.float32)
        grad_mid = norm_back(normed, scaling, cot_rows[targets]).astype(jnp.bfloat16)
        grad_pre = (matmul_t(grad_mid, w_proc2) * silu_slope(preact)).astype(jnp.bfloat16)
        flat_pre = grad_pre.reshape(-1, D)
        g_lookup = jax.ops.segment_sum(matmul_t(flat_pre, w_src), sources.reshape(-1), num_segments=table_rows)
        g_node = cot_rows + g_lookup[:part_rows] + jax.ops.segment_sum(matmul_t(flat_pre, w_dst), targets.reshape(-1), num_segments=part_rows)
        pieces = (outer_batch(hidden, grad_mid), outer_batch(src_rows, grad_pre), outer_batch(dst_rows, grad_pre))
        carry = (carry[0] + rounded_sum(pieces[0]), carry[1] + rounded_sum(pieces[1]), carry[2] + rounded_sum(pieces[2]))
        return (carry, (out_part, g_node, g_lookup[part_rows:].reshape(N_DOM, HCAP, D)))
    proc_sums, (out_all, g_node_all, g_halo_all) = lax.scan(process, (zero_square, zero_square, zero_square), dom_ids)
    back_idx = jnp.transpose(hal_idx, (1, 0, 2))
    segment = dom_ids[None, :, None] * part_rows + jnp.maximum(back_idx, 0)
    contrib = jnp.where((back_idx >= 0)[..., None], g_halo_all, jnp.zeros_like(g_halo_all))
    node_grad = g_node_all.reshape(N_DOM * part_rows, D) + jax.ops.segment_sum(contrib.reshape(-1, D), segment.reshape(-1), num_segments=N_DOM * part_rows)
    node_grad = node_grad.reshape(N_DOM, part_rows, D)

    def encode_back(carry, dom_index):
        mesh_part, targets, valid, preact, hidden, normed, scaling = encoder_values(dom_index)
        g_nodes = node_grad[dom_index]
        grad_mid = norm_back(normed, scaling, g_nodes[targets] * valid).astype(jnp.bfloat16)
        grad_pre = (matmul_t(grad_mid, w_enc2) * silu_slope(preact)).astype(jnp.bfloat16)
        back_mesh = jax.ops.segment_sum(matmul_t(grad_pre.reshape(-1, D), w_mesh), targets.reshape(-1), num_segments=part_rows)
        g_mesh_part = (g_nodes + back_mesh).astype(jnp.bfloat16)
        carry = (carry[0] + rounded_sum(outer_batch(hidden, grad_mid)), carry[1] + rounded_sum(outer_batch(mesh_part[targets], grad_pre)))
        return (carry, (g_mesh_part, grad_pre.reshape(N_FEAT, N_DOM, CAP, D)))
    enc_sums, (g_mesh_all, returned) = lax.scan(encode_back, (zero_square, zero_square), dom_ids)

    def segment_rows(values, indices):
        return jax.ops.segment_sum(values, indices, num_segments=G_DEV)

    def send_back(carry, dom_index):
        grads = jnp.transpose(returned[:, :, dom_index], (1, 0, 2, 3)).reshape(N_FEAT, N_DOM * CAP, D)
        devices = dom_index * N_FEAT + feat_ids
        rows_idx = send_idx[devices].reshape(N_FEAT, N_DOM * CAP)
        row_pick = jnp.maximum(rows_idx, 0)
        grid_rows = grid_dev[devices[:, None], row_pick]
        back_rows = matmul_t(grads, w_grid) * (rows_idx >= 0).astype(jnp.float32)[..., None]
        g_grid_part = jax.vmap(segment_rows)(back_rows, row_pick).astype(jnp.bfloat16)
        return (carry + rounded_sum(outer_batch(grid_rows, grads)), g_grid_part)
    grid_sum, g_grid_all = lax.scan(send_back, zero_square, dom_ids)
    return (out_all.reshape(N_DOM * part_rows, D), g_grid_all.reshape(device_count * G_DEV, D), g_mesh_all.reshape(N_DOM * part_rows, D), factor * grid_sum, factor * enc_sums[1], factor * enc_sums[0], factor * proc_sums[1], factor * proc_sums[2], factor * proc_sums[0])
```

```python
import functools
import math

import jax
import jax.numpy as jnp
from jax import lax
from jax.experimental import pallas as pl
from jax.experimental.pallas import tpu as pltpu
from jax.sharding import PartitionSpec as P

EPS = 1e-05
BF16 = jnp.bfloat16
F32 = jnp.float32
MESH_ID = pl.DeviceIdType.MESH
SLAB = 8
TILE = 16


def matmul(left, right):
    return jnp.dot(left, right, preferred_element_type=jnp.float32)


def matmul_t(left, right):
    return lax.dot_general(
        left, right, (((left.ndim - 1,), (1,)), ((), ())), preferred_element_type=jnp.float32
    )


def outer(left, right):
    return lax.dot_general(
        left, right, (((0,), (0,)), ((), ())), preferred_element_type=jnp.float32
    )


def layer_norm(values):
    center = values - jnp.mean(values, axis=-1, keepdims=True)
    spread = jnp.mean(center * center, axis=-1, keepdims=True)
    scaling = lax.rsqrt(spread + EPS)
    return (center * scaling, scaling)


def norm_back(normed, scaling, upstream):
    inner = jnp.mean(upstream, axis=-1, keepdims=True)
    along = jnp.mean(upstream * normed, axis=-1, keepdims=True)
    return scaling * (upstream - inner - normed * along)


def silu_slope(preact):
    sigma = jax.nn.sigmoid(preact)
    return sigma * (1.0 + preact * (1.0 - sigma))


def edge_forward(preact, weight):
    hidden = jax.nn.silu(preact).astype(jnp.bfloat16)
    normed, scaling = layer_norm(matmul(hidden, weight))
    return (hidden, normed, scaling)


def pick_rows(source, indices):
    chosen = source[jnp.maximum(indices, 0)]
    return jnp.where((indices >= 0)[..., None], chosen, jnp.zeros((), source.dtype))


def per_device(
    grid_feat,
    mesh_feat,
    w_grid,
    w_mesh,
    w_enc2,
    w_src,
    w_dst,
    w_proc2,
    enc_send,
    enc_dst,
    hal_send,
    proc_src,
    proc_dst,
    cotangent,
):
    dom_count = lax.axis_size("dom")
    feat_count = lax.axis_size("feat")
    own_rows = mesh_feat.shape[0]
    latent_width = grid_feat.shape[1]
    part_rows = own_rows * feat_count
    slot_count = enc_send.shape[1]
    halo_count = hal_send.shape[1]
    factor = 1.0 / math.sqrt(own_rows * dom_count * feat_count)
    gathered = (
        lax.all_gather(w_grid, "feat", axis=0, tiled=True),
        lax.all_gather(w_mesh, "feat", axis=0, tiled=True),
        lax.all_gather(w_enc2, "feat", axis=0, tiled=True),
        lax.all_gather(w_src, "feat", axis=0, tiled=True),
        lax.all_gather(w_dst, "feat", axis=0, tiled=True),
        lax.all_gather(w_proc2, "feat", axis=0, tiled=True),
        lax.all_gather(mesh_feat, "feat", axis=0, tiled=True),
        lax.all_gather(cotangent, "feat", axis=0, tiled=True),
    )
    full_grid, full_mesh, full_enc2, full_src, full_dst, full_proc2, mesh_part, cot_part = gathered
    own_start = lax.axis_index("feat") * own_rows
    projected = matmul(grid_feat, full_grid).astype(jnp.bfloat16)
    outgoing = pick_rows(projected, enc_send)
    received = lax.all_to_all(outgoing, "dom", split_axis=0, concat_axis=0, tiled=True)
    node_proj = matmul(mesh_part, full_mesh)
    targets = jnp.maximum(enc_dst, 0).reshape(-1)
    valid = (enc_dst >= 0).reshape(-1, 1).astype(jnp.float32)
    preact = received.reshape(-1, latent_width).astype(jnp.float32) + node_proj[targets]
    hidden, normed, scaling = edge_forward(preact, full_enc2)
    partial_value = jax.ops.segment_sum(normed * valid, targets, num_segments=part_rows)
    summed = lax.psum(partial_value, "feat")
    latent = (mesh_part.astype(jnp.float32) + summed).astype(jnp.bfloat16)
    halo_rows = lax.all_to_all(
        pick_rows(latent, hal_send), "dom", split_axis=0, concat_axis=0, tiled=True
    )
    lookup = jnp.concatenate([latent, halo_rows.reshape(-1, latent_width)], axis=0)
    src_rows = lookup[proc_src]
    dst_rows = latent[proc_dst]
    preact_p = matmul(src_rows, full_src) + matmul(dst_rows, full_dst)
    hidden_p, normed_p, scaling_p = edge_forward(preact_p, full_proc2)
    partial_p = jax.ops.segment_sum(normed_p, proc_dst, num_segments=part_rows)
    summed_p = lax.psum(partial_p, "feat")
    result = (latent.astype(jnp.float32) + summed_p).astype(jnp.bfloat16)
    out_rows = lax.dynamic_slice_in_dim(result, own_start, own_rows, 0)
    cot_rows = cot_part.astype(jnp.float32)
    grad_mid_p = norm_back(normed_p, scaling_p, cot_rows[proc_dst]).astype(jnp.bfloat16)
    grad_pre_p = (matmul_t(grad_mid_p, full_proc2) * silu_slope(preact_p)).astype(jnp.bfloat16)
    g_lookup = jax.ops.segment_sum(
        matmul_t(grad_pre_p, full_src), proc_src, num_segments=lookup.shape[0]
    )
    g_local = g_lookup[:part_rows] + jax.ops.segment_sum(
        matmul_t(grad_pre_p, full_dst), proc_dst, num_segments=part_rows
    )
    halo_back = g_lookup[part_rows:].reshape(dom_count, halo_count, latent_width)
    returned = lax.all_to_all(halo_back, "dom", split_axis=0, concat_axis=0, tiled=True)
    returned = jnp.where((hal_send >= 0)[..., None], returned, jnp.zeros((), jnp.float32))
    g_local = g_local + jax.ops.segment_sum(
        returned.reshape(-1, latent_width),
        jnp.maximum(hal_send, 0).reshape(-1),
        num_segments=part_rows,
    )
    node_grad = lax.psum(g_local, "feat") + cot_rows
    grad_mid_e = norm_back(normed, scaling, node_grad[targets] * valid).astype(jnp.bfloat16)
    grad_pre_e = (matmul_t(grad_mid_e, full_enc2) * silu_slope(preact)).astype(jnp.bfloat16)
    mesh_back = jax.ops.segment_sum(
        matmul_t(grad_pre_e, full_mesh), targets, num_segments=part_rows
    )
    mesh_share = lax.psum_scatter(mesh_back, "feat", scatter_dimension=0, tiled=True)
    own_grad = lax.dynamic_slice_in_dim(node_grad, own_start, own_rows, 0)
    g_mesh = (own_grad + mesh_share).astype(jnp.bfloat16)
    slot_back = lax.all_to_all(
        grad_pre_e.reshape(dom_count, slot_count, latent_width),
        "dom",
        split_axis=0,
        concat_axis=0,
        tiled=True,
    )
    send_rows = jnp.maximum(enc_send, 0).reshape(-1)
    send_live = (enc_send >= 0).reshape(-1, 1).astype(jnp.float32)
    flat_back = slot_back.reshape(-1, latent_width)
    grid_back = matmul_t(flat_back, full_grid) * send_live
    g_grid = jax.ops.segment_sum(grid_back, send_rows, num_segments=grid_feat.shape[0]).astype(
        jnp.bfloat16
    )
    terms = (
        outer(grid_feat[send_rows], flat_back),
        outer(mesh_part[targets], grad_pre_e),
        outer(hidden, grad_mid_e),
        outer(src_rows, grad_pre_p),
        outer(dst_rows, grad_pre_p),
        outer(hidden_p, grad_mid_p),
    )
    shares = (
        lax.psum_scatter(
            terms[0].astype(jnp.bfloat16), "feat", scatter_dimension=0, tiled=True
        ).astype(jnp.float32),
        lax.psum_scatter(
            terms[1].astype(jnp.bfloat16), "feat", scatter_dimension=0, tiled=True
        ).astype(jnp.float32),
        lax.psum_scatter(
            terms[2].astype(jnp.bfloat16), "feat", scatter_dimension=0, tiled=True
        ).astype(jnp.float32),
        lax.psum_scatter(
            terms[3].astype(jnp.bfloat16), "feat", scatter_dimension=0, tiled=True
        ).astype(jnp.float32),
        lax.psum_scatter(
            terms[4].astype(jnp.bfloat16), "feat", scatter_dimension=0, tiled=True
        ).astype(jnp.float32),
        lax.psum_scatter(
            terms[5].astype(jnp.bfloat16), "feat", scatter_dimension=0, tiled=True
        ).astype(jnp.float32),
    )
    totals = lax.psum((shares[0], shares[1], shares[2], shares[3], shares[4], shares[5]), "dom")
    return (
        out_rows,
        g_grid,
        g_mesh,
        factor * totals[0],
        factor * totals[1],
        factor * totals[2],
        factor * totals[3],
        factor * totals[4],
        factor * totals[5],
    )


def pick(hot, rows):
    return matmul(hot, rows).astype(BF16)


def halves(values):
    high = values.astype(BF16)
    return (high, (values - high.astype(F32)).astype(BF16))


def pick_wide(hot, values):
    high, low = halves(values)
    return matmul(hot, high) + matmul(hot, low)


def spread(hot, values):
    high, low = halves(values)
    return outer(hot, high) + outer(hot, low)


def hot_rows(indices, width):
    columns = lax.broadcasted_iota(jnp.int32, (indices.shape[0], width), 1)
    return jnp.where(columns == indices, 1.0, 0.0).astype(BF16)


def hidden_and_slope(preact):
    sigma = 1.0 / (1.0 + jnp.exp(-preact))
    return ((preact * sigma).astype(BF16), sigma * (1.0 + preact * (1.0 - sigma)))


def fused_kernel(
    sizes,
    grid_ref,
    mesh_ref,
    wg_ref,
    wm_ref,
    we_ref,
    ws_ref,
    wd_ref,
    wp_ref,
    index_ref,
    cot_ref,
    out_ref,
    ggrid_ref,
    gmesh_ref,
    o_wg,
    o_wm,
    o_we,
    o_ws,
    o_wd,
    o_wp,
    weights,
    mesh_buf,
    cot_buf,
    slot_out,
    slot_in,
    halo_out,
    halo_in,
    halo_bout,
    halo_bin,
    slot_bout,
    slot_bin,
    sum_buf,
    share_out,
    share_in,
    term,
    pair_in,
    cross_out,
    cross_in,
    ring_out,
    ring_in,
    total_buf,
    gather_sems,
    dom_sems,
    sum_sems,
    share_sems,
    pair_sems,
    cross_sems,
):
    dom, feat, own, part, edges = sizes
    me = lax.axis_index("dom")
    f = lax.axis_index("feat")
    f1 = f + 1 - 2 * lax.rem(f, 2)
    f2 = lax.rem(f + 2, feat)
    f3 = lax.rem(f1 + 2, feat)
    factor = 1.0 / math.sqrt(own * dom * feat)

    def send(src, dst, sems, slot, **where):
        copy = pltpu.make_async_remote_copy(
            src_ref=src,
            dst_ref=dst,
            send_sem=sems.at[(0,) + slot],
            recv_sem=sems.at[(1,) + slot],
            device_id=where,
            device_id_type=MESH_ID,
        )
        copy.start()
        return copy

    def finish(copies):
        for copy in copies:
            copy.wait()

    def dom_exchange(kind, src, dst):
        copies = []
        for step in range(1, dom):
            peer = lax.rem(me + step, dom)
            copies.append(send(src.at[peer], dst.at[me], dom_sems, (kind, step), dom=peer))
        dst[me] = src[me]
        return copies

    def put_slabs(ref, rows):
        for index in range(dom):
            ref[index] = rows[index * SLAB : (index + 1) * SLAB].astype(BF16)

    def get_slabs(ref):
        return jnp.concatenate([ref[index].astype(F32) for index in range(dom)], axis=0).astype(BF16)

    def all_parts(ref):
        return jnp.concatenate([ref[index].astype(F32) for index in range(feat)], axis=0)

    barrier = pltpu.get_barrier_semaphore()
    for step in range(1, dom):
        pl.semaphore_signal(
            barrier, inc=1, device_id={"dom": lax.rem(me + step, dom)}, device_id_type=MESH_ID
        )
    for step in range(1, feat):
        pl.semaphore_signal(
            barrier, inc=1, device_id={"feat": lax.rem(f + step, feat)}, device_id_type=MESH_ID
        )
    mesh_buf[f] = mesh_ref[...]
    cot_buf[f] = cot_ref[...]
    slots = dom * SLAB
    send_hot = hot_rows(index_ref[0:slots], grid_ref.shape[0])
    put_slabs(slot_out, matmul(send_hot, grid_ref[...]))
    pl.semaphore_wait(barrier, dom + feat - 2)

    slot_copies = dom_exchange(0, slot_out, slot_in)
    pieces = [
        (wg_ref, lambda g: weights.at[0, g]),
        (mesh_buf.at[f], lambda g: mesh_buf.at[g]),
        (wm_ref, lambda g: weights.at[1, g]),
        (we_ref, lambda g: weights.at[2, g]),
        (ws_ref, lambda g: weights.at[3, g]),
        (wd_ref, lambda g: weights.at[4, g]),
        (wp_ref, lambda g: weights.at[5, g]),
        (cot_buf.at[f], lambda g: cot_buf.at[g]),
    ]
    across, beside, passed = [], [], []
    for slot, (src, dst) in enumerate(pieces):
        across.append(send(src, dst(f), gather_sems, (0, slot), feat=f2))
        beside.append(send(src, dst(f), gather_sems, (1, slot), feat=f1))
    for slot, src in enumerate((wg_ref, wm_ref, we_ref, ws_ref, wd_ref, wp_ref)):
        weights[slot, f] = src[...]
    for slot, (src, dst) in enumerate(pieces):
        across[slot].wait_recv()
        passed.append(send(dst(f2), dst(f2), gather_sems, (2, slot), feat=f1))

    def whole(slot):
        return weights[slot].reshape(feat * weights.shape[2], weights.shape[3])

    def arrived(slot):
        beside[slot].wait_recv()
        passed[slot].wait_recv()

    target_hot = hot_rows(index_ref[slots : 2 * slots], part)
    finish(slot_copies)
    grid_rows = get_slabs(slot_in)
    for slot in (0, 1, 2, 3):
        arrived(slot)
    mesh_part = all_parts(mesh_buf)
    mesh_rows = pick(target_hot, mesh_part.astype(BF16))
    preact_e = pick(grid_rows, whole(0)).astype(F32) + matmul(mesh_rows, whole(1))
    hidden_e, slope_e = hidden_and_slope(preact_e)
    normed_e, scaling_e = layer_norm(matmul(hidden_e, whole(2)))

    def feat_sum(kind, value):
        first = value.astype(BF16)
        sum_buf[kind, 0] = first
        copy = send(sum_buf.at[kind, 0], sum_buf.at[kind, 1], sum_sems, (kind, 0), feat=f1)
        yield
        copy.wait()
        both = (first.astype(F32) + sum_buf[kind, 1].astype(F32)).astype(BF16)
        sum_buf[kind, 2] = both
        copy = send(sum_buf.at[kind, 2], sum_buf.at[kind, 3], sum_sems, (kind, 1), feat=f2)
        yield
        copy.wait()
        yield both.astype(F32) + sum_buf[kind, 3].astype(F32)

    stages = feat_sum(0, spread(target_hot, normed_e))
    next(stages)
    next(stages)
    halo_hot = hot_rows(index_ref[2 * slots : 3 * slots], part)
    source_hot = hot_rows(index_ref[3 * slots : 3 * slots + edges], part + slots)
    edge_hot = hot_rows(index_ref[3 * slots + edges : 3 * slots + 2 * edges], part)
    latent = (mesh_part + next(stages)).astype(BF16)

    put_slabs(halo_out, matmul(halo_hot, latent))
    halo_copies = dom_exchange(1, halo_out, halo_in)
    dst_rows = pick(edge_hot, latent)
    for slot in (4, 5, 6, 7):
        arrived(slot)
    pre_dst = matmul(dst_rows, whole(4))
    upstream_p = matmul(edge_hot, all_parts(cot_buf).astype(BF16))
    finish(halo_copies)
    lookup = jnp.concatenate([latent, get_slabs(halo_in)], axis=0)
    src_rows = pick(source_hot, lookup)
    preact_p = matmul(src_rows, whole(3)) + pre_dst
    hidden_p, slope_p = hidden_and_slope(preact_p)
    normed_p, scaling_p = layer_norm(matmul(hidden_p, whole(5)))

    mid_p = norm_back(normed_p, scaling_p, upstream_p).astype(BF16)
    grad_p = (matmul_t(mid_p, whole(5)) * slope_p).astype(BF16)
    g_lookup = spread(source_hot, matmul_t(grad_p, whole(3)))
    put_slabs(halo_bout, g_lookup[part:])
    back_copies = dom_exchange(2, halo_bout, halo_bin)
    g_local = g_lookup[:part] + spread(edge_hot, matmul_t(grad_p, whole(4)))

    def scatter_own(kind, value):
        for index in range(feat):
            share_out[kind, index] = value[index * own : (index + 1) * own].astype(BF16)
        copies = []
        for step in range(1, feat):
            peer = lax.rem(f + step, feat)
            copies.append(
                send(
                    share_out.at[kind, peer],
                    share_in.at[kind, f],
                    share_sems,
                    (kind, step),
                    feat=peer,
                )
            )
        share_in[kind, f] = share_out[kind, f]
        return copies

    def own_sum(kind):
        total = share_in[kind, 0].astype(F32)
        for index in range(1, feat):
            total = total + share_in[kind, index].astype(F32)
        return total

    rows = term.shape[3]
    chunk = ring_out.shape[3]

    def start_terms(group, left, right):
        for index in range(3):
            product = outer(left[index], right[index]).astype(BF16)
            for shard in range(feat):
                term[group, shard, index] = product[shard * rows : (shard + 1) * rows]
        return [
            send(term.at[group, f1], pair_in.at[group, 0], pair_sems, (group, 0), feat=f1),
            send(term.at[group, f3], pair_in.at[group, 1], pair_sems, (group, 1), feat=f1),
        ]

    def cross_terms(group, copies):
        finish(copies)
        for index in range(3):
            cross_out[group, index] = (
                term[group, f2, index].astype(F32) + pair_in[group, 1, index].astype(F32)
            ).astype(BF16)
        return [send(cross_out.at[group], cross_in.at[group], cross_sems, (group,), feat=f2)]

    def ring_terms(group, copies):
        finish(copies)
        for index in range(3):
            share = (
                term[group, f, index].astype(F32)
                + pair_in[group, 0, index].astype(F32)
                + cross_in[group, index].astype(F32)
            ).astype(BF16)
            for piece in range(dom):
                ring_out[group, piece, index] = share[piece * chunk : (piece + 1) * chunk]
        return dom_exchange(4 + 2 * group, ring_out.at[group], ring_in.at[group])

    def total_terms(group, copies):
        finish(copies)
        for index in range(3):
            total = ring_in[group, 0, index].astype(F32)
            for piece in range(1, dom):
                total = total + ring_in[group, piece, index].astype(F32)
            total_buf[group, me, index] = total.astype(BF16)
        copies = []
        for step in range(1, dom):
            peer = lax.rem(me + step, dom)
            copies.append(
                send(
                    total_buf.at[group, me],
                    total_buf.at[group, me],
                    dom_sems,
                    (5 + 2 * group, step),
                    dom=peer,
                )
            )
        return copies

    def write_terms(group, copies, refs):
        finish(copies)
        for index, ref in enumerate(refs):
            for piece in range(dom):
                ref[piece * chunk : (piece + 1) * chunk] = factor * total_buf[
                    group, piece, index
                ].astype(F32)

    proc_pair = start_terms(0, (src_rows, dst_rows, hidden_p), (grad_p, grad_p, mid_p))
    finish(back_copies)
    g_local = g_local + outer(halo_hot, get_slabs(halo_bin))
    stages = feat_sum(1, g_local)
    next(stages)
    next(stages)
    proc_share = scatter_own(0, spread(edge_hot, normed_p))
    proc_cross = cross_terms(0, proc_pair)
    cot_part = all_parts(cot_buf)
    node_grad = next(stages) + cot_part

    mid_e = norm_back(normed_e, scaling_e, pick_wide(target_hot, node_grad)).astype(BF16)
    grad_e = (matmul_t(mid_e, whole(2)) * slope_e).astype(BF16)
    enc_pair = start_terms(1, (grid_rows, mesh_rows, hidden_e), (grad_e, grad_e, mid_e))
    put_slabs(slot_bout, grad_e.astype(F32))
    slot_copies = dom_exchange(3, slot_bout, slot_bin)
    enc_share = scatter_own(1, spread(target_hot, matmul_t(grad_e, whole(1))))
    enc_cross = cross_terms(1, enc_pair)
    proc_ring = ring_terms(0, proc_cross)
    own_hot = hot_rows(
        f * own + lax.broadcasted_iota(jnp.int32, (own, 1), 0), part
    )
    own_grad = pick_wide(own_hot, node_grad)
    own_latent = matmul(own_hot, latent)
    finish(slot_copies)
    slot_rows = outer(send_hot, get_slabs(slot_bin)).astype(BF16)
    ggrid_ref[...] = matmul_t(slot_rows, whole(0)).astype(BF16)
    finish(proc_share)
    out_ref[...] = (own_latent + own_sum(0)).astype(BF16)
    proc_total = total_terms(0, proc_ring)
    enc_ring = ring_terms(1, enc_cross)
    finish(enc_share)
    gmesh_ref[...] = (own_grad + own_sum(1)).astype(BF16)
    enc_total = total_terms(1, enc_ring)
    write_terms(0, proc_total, (o_ws, o_wd, o_wp))
    write_terms(1, enc_total, (o_wg, o_wm, o_we))
    for copies in (across, beside, passed):
        for copy in copies:
            copy.wait_send()


def fused(
    grid_feat,
    mesh_feat,
    w_grid,
    w_mesh,
    w_enc2,
    w_src,
    w_dst,
    w_proc2,
    enc_send,
    enc_dst,
    hal_send,
    proc_src,
    proc_dst,
    cotangent,
):
    dom = lax.axis_size("dom")
    feat = lax.axis_size("feat")
    own, width = mesh_feat.shape
    part = own * feat
    edges = proc_src.shape[0]
    halo = hal_send.shape[1]
    shard = w_grid.shape[0]
    chunk = shard // dom

    def slabs(table):
        return jnp.pad(table, ((0, 0), (0, SLAB - table.shape[1])), constant_values=-1).reshape(-1)

    far = proc_src - part
    moved = jnp.where(far < 0, proc_src, part + far // halo * SLAB + far % halo)
    indices = jnp.concatenate([slabs(enc_send), slabs(enc_dst), slabs(hal_send), moved, proc_dst])
    slab = pltpu.VMEM((dom, SLAB, width), BF16)
    vmem = pl.BlockSpec(memory_space=pltpu.VMEM)
    weight_out = jax.ShapeDtypeStruct((shard, width), F32)
    return pl.pallas_call(
        functools.partial(fused_kernel, (dom, feat, own, part, edges)),
        out_shape=(
            jax.ShapeDtypeStruct((own, width), BF16),
            jax.ShapeDtypeStruct(grid_feat.shape, BF16),
            jax.ShapeDtypeStruct((own, width), BF16),
        )
        + (weight_out,) * 6,
        in_specs=[vmem] * 10,
        out_specs=(vmem,) * 9,
        scratch_shapes=[
            pltpu.VMEM((6, feat, shard, width), BF16),
            pltpu.VMEM((feat, own, width), BF16),
            pltpu.VMEM((feat, own, width), BF16),
            slab,
            slab,
            slab,
            slab,
            slab,
            slab,
            slab,
            slab,
            pltpu.VMEM((2, 4, part, width), BF16),
            pltpu.VMEM((2, feat, own, width), BF16),
            pltpu.VMEM((2, feat, own, width), BF16),
            pltpu.VMEM((2, feat, 3, shard, width), BF16),
            pltpu.VMEM((2, 2, 3, shard, width), BF16),
            pltpu.VMEM((2, 3, shard, width), BF16),
            pltpu.VMEM((2, 3, shard, width), BF16),
            pltpu.VMEM((2, dom, 3, chunk, width), BF16),
            pltpu.VMEM((2, dom, 3, chunk, width), BF16),
            pltpu.VMEM((2, dom, 3, chunk, width), BF16),
            pltpu.SemaphoreType.DMA((2, 3, 8)),
            pltpu.SemaphoreType.DMA((2, 8, dom)),
            pltpu.SemaphoreType.DMA((2, 2, 2)),
            pltpu.SemaphoreType.DMA((2, 2, feat)),
            pltpu.SemaphoreType.DMA((2, 2, 2)),
            pltpu.SemaphoreType.DMA((2, 2)),
        ],
        compiler_params=pltpu.CompilerParams(
            collective_id=0, has_side_effects=True, vmem_limit_bytes=56 * 1024 * 1024
        ),
        name="fused_layer",
    )(
        grid_feat,
        mesh_feat,
        w_grid,
        w_mesh,
        w_enc2,
        w_src,
        w_dst,
        w_proc2,
        indices[:, None],
        cotangent,
    )


def choose(*args):
    dom = lax.axis_size("dom")
    feat = lax.axis_size("feat")
    shard = args[2].shape[0]
    fits = max(args[8].shape[1], args[10].shape[1]) <= SLAB
    if feat == 4 and shard % (dom * TILE) == 0 and fits:
        return fused(*args)
    return per_device(*args)


def solution(mesh):
    return jax.shard_map(
        choose,
        mesh=mesh,
        in_specs=(
            P(("dom", "feat"), None),
            P(("dom", "feat"), None),
            P("feat", None),
            P("feat", None),
            P("feat", None),
            P("feat", None),
            P("feat", None),
            P("feat", None),
            P(("dom", "feat"), None),
            P(("dom", "feat"), None),
            P("dom", None),
            P(("dom", "feat")),
            P(("dom", "feat")),
            P(("dom", "feat"), None),
        ),
        out_specs=(
            P(("dom", "feat"), None),
            P(("dom", "feat"), None),
            P(("dom", "feat"), None),
            P("feat", None),
            P("feat", None),
            P("feat", None),
            P("feat", None),
            P("feat", None),
            P("feat", None),
        ),
        check_vma=False,
    )
```

```python
import functools
import math

import jax
import jax.numpy as jnp
from jax import lax
from jax.experimental import pallas as pl
from jax.experimental.pallas import tpu as pltpu
from jax.sharding import PartitionSpec as P

EPS = 1e-05
BF16 = jnp.bfloat16
F32 = jnp.float32
MESH_ID = pl.DeviceIdType.MESH
SLAB = 8
TILE = 16


def matmul(left, right):
    return jnp.dot(left, right, preferred_element_type=jnp.float32)


def matmul_t(left, right):
    return lax.dot_general(
        left, right, (((left.ndim - 1,), (1,)), ((), ())), preferred_element_type=jnp.float32
    )


def outer(left, right):
    return lax.dot_general(
        left, right, (((0,), (0,)), ((), ())), preferred_element_type=jnp.float32
    )


def layer_norm(values):
    center = values - jnp.mean(values, axis=-1, keepdims=True)
    spread = jnp.mean(center * center, axis=-1, keepdims=True)
    scaling = lax.rsqrt(spread + EPS)
    return (center * scaling, scaling)


def norm_back(normed, scaling, upstream):
    inner = jnp.mean(upstream, axis=-1, keepdims=True)
    along = jnp.mean(upstream * normed, axis=-1, keepdims=True)
    return scaling * (upstream - inner - normed * along)


def silu_slope(preact):
    sigma = jax.nn.sigmoid(preact)
    return sigma * (1.0 + preact * (1.0 - sigma))


def edge_forward(preact, weight):
    hidden = jax.nn.silu(preact).astype(jnp.bfloat16)
    normed, scaling = layer_norm(matmul(hidden, weight))
    return (hidden, normed, scaling)


def pick_rows(source, indices):
    chosen = source[jnp.maximum(indices, 0)]
    return jnp.where((indices >= 0)[..., None], chosen, jnp.zeros((), source.dtype))


def per_device(
    grid_feat,
    mesh_feat,
    w_grid,
    w_mesh,
    w_enc2,
    w_src,
    w_dst,
    w_proc2,
    enc_send,
    enc_dst,
    hal_send,
    proc_src,
    proc_dst,
    cotangent,
):
    dom_count = lax.axis_size("dom")
    feat_count = lax.axis_size("feat")
    own_rows = mesh_feat.shape[0]
    latent_width = grid_feat.shape[1]
    part_rows = own_rows * feat_count
    slot_count = enc_send.shape[1]
    halo_count = hal_send.shape[1]
    factor = 1.0 / math.sqrt(own_rows * dom_count * feat_count)
    gathered = (
        lax.all_gather(w_grid, "feat", axis=0, tiled=True),
        lax.all_gather(w_mesh, "feat", axis=0, tiled=True),
        lax.all_gather(w_enc2, "feat", axis=0, tiled=True),
        lax.all_gather(w_src, "feat", axis=0, tiled=True),
        lax.all_gather(w_dst, "feat", axis=0, tiled=True),
        lax.all_gather(w_proc2, "feat", axis=0, tiled=True),
        lax.all_gather(mesh_feat, "feat", axis=0, tiled=True),
        lax.all_gather(cotangent, "feat", axis=0, tiled=True),
    )
    full_grid, full_mesh, full_enc2, full_src, full_dst, full_proc2, mesh_part, cot_part = gathered
    own_start = lax.axis_index("feat") * own_rows
    projected = matmul(grid_feat, full_grid).astype(jnp.bfloat16)
    outgoing = pick_rows(projected, enc_send)
    received = lax.all_to_all(outgoing, "dom", split_axis=0, concat_axis=0, tiled=True)
    node_proj = matmul(mesh_part, full_mesh)
    targets = jnp.maximum(enc_dst, 0).reshape(-1)
    valid = (enc_dst >= 0).reshape(-1, 1).astype(jnp.float32)
    preact = received.reshape(-1, latent_width).astype(jnp.float32) + node_proj[targets]
    hidden, normed, scaling = edge_forward(preact, full_enc2)
    partial_value = jax.ops.segment_sum(normed * valid, targets, num_segments=part_rows)
    summed = lax.psum(partial_value, "feat")
    latent = (mesh_part.astype(jnp.float32) + summed).astype(jnp.bfloat16)
    halo_rows = lax.all_to_all(
        pick_rows(latent, hal_send), "dom", split_axis=0, concat_axis=0, tiled=True
    )
    lookup = jnp.concatenate([latent, halo_rows.reshape(-1, latent_width)], axis=0)
    src_rows = lookup[proc_src]
    dst_rows = latent[proc_dst]
    preact_p = matmul(src_rows, full_src) + matmul(dst_rows, full_dst)
    hidden_p, normed_p, scaling_p = edge_forward(preact_p, full_proc2)
    partial_p = jax.ops.segment_sum(normed_p, proc_dst, num_segments=part_rows)
    summed_p = lax.psum(partial_p, "feat")
    result = (latent.astype(jnp.float32) + summed_p).astype(jnp.bfloat16)
    out_rows = lax.dynamic_slice_in_dim(result, own_start, own_rows, 0)
    cot_rows = cot_part.astype(jnp.float32)
    grad_mid_p = norm_back(normed_p, scaling_p, cot_rows[proc_dst]).astype(jnp.bfloat16)
    grad_pre_p = (matmul_t(grad_mid_p, full_proc2) * silu_slope(preact_p)).astype(jnp.bfloat16)
    g_lookup = jax.ops.segment_sum(
        matmul_t(grad_pre_p, full_src), proc_src, num_segments=lookup.shape[0]
    )
    g_local = g_lookup[:part_rows] + jax.ops.segment_sum(
        matmul_t(grad_pre_p, full_dst), proc_dst, num_segments=part_rows
    )
    halo_back = g_lookup[part_rows:].reshape(dom_count, halo_count, latent_width)
    returned = lax.all_to_all(halo_back, "dom", split_axis=0, concat_axis=0, tiled=True)
    returned = jnp.where((hal_send >= 0)[..., None], returned, jnp.zeros((), jnp.float32))
    g_local = g_local + jax.ops.segment_sum(
        returned.reshape(-1, latent_width),
        jnp.maximum(hal_send, 0).reshape(-1),
        num_segments=part_rows,
    )
    node_grad = lax.psum(g_local, "feat") + cot_rows
    grad_mid_e = norm_back(normed, scaling, node_grad[targets] * valid).astype(jnp.bfloat16)
    grad_pre_e = (matmul_t(grad_mid_e, full_enc2) * silu_slope(preact)).astype(jnp.bfloat16)
    mesh_back = jax.ops.segment_sum(
        matmul_t(grad_pre_e, full_mesh), targets, num_segments=part_rows
    )
    mesh_share = lax.psum_scatter(mesh_back, "feat", scatter_dimension=0, tiled=True)
    own_grad = lax.dynamic_slice_in_dim(node_grad, own_start, own_rows, 0)
    g_mesh = (own_grad + mesh_share).astype(jnp.bfloat16)
    slot_back = lax.all_to_all(
        grad_pre_e.reshape(dom_count, slot_count, latent_width),
        "dom",
        split_axis=0,
        concat_axis=0,
        tiled=True,
    )
    send_rows = jnp.maximum(enc_send, 0).reshape(-1)
    send_live = (enc_send >= 0).reshape(-1, 1).astype(jnp.float32)
    flat_back = slot_back.reshape(-1, latent_width)
    grid_back = matmul_t(flat_back, full_grid) * send_live
    g_grid = jax.ops.segment_sum(grid_back, send_rows, num_segments=grid_feat.shape[0]).astype(
        jnp.bfloat16
    )
    terms = (
        outer(grid_feat[send_rows], flat_back),
        outer(mesh_part[targets], grad_pre_e),
        outer(hidden, grad_mid_e),
        outer(src_rows, grad_pre_p),
        outer(dst_rows, grad_pre_p),
        outer(hidden_p, grad_mid_p),
    )
    shares = (
        lax.psum_scatter(
            terms[0].astype(jnp.bfloat16), "feat", scatter_dimension=0, tiled=True
        ).astype(jnp.float32),
        lax.psum_scatter(
            terms[1].astype(jnp.bfloat16), "feat", scatter_dimension=0, tiled=True
        ).astype(jnp.float32),
        lax.psum_scatter(
            terms[2].astype(jnp.bfloat16), "feat", scatter_dimension=0, tiled=True
        ).astype(jnp.float32),
        lax.psum_scatter(
            terms[3].astype(jnp.bfloat16), "feat", scatter_dimension=0, tiled=True
        ).astype(jnp.float32),
        lax.psum_scatter(
            terms[4].astype(jnp.bfloat16), "feat", scatter_dimension=0, tiled=True
        ).astype(jnp.float32),
        lax.psum_scatter(
            terms[5].astype(jnp.bfloat16), "feat", scatter_dimension=0, tiled=True
        ).astype(jnp.float32),
    )
    totals = lax.psum((shares[0], shares[1], shares[2], shares[3], shares[4], shares[5]), "dom")
    return (
        out_rows,
        g_grid,
        g_mesh,
        factor * totals[0],
        factor * totals[1],
        factor * totals[2],
        factor * totals[3],
        factor * totals[4],
        factor * totals[5],
    )


def pick(hot, rows):
    return matmul(hot, rows).astype(BF16)


def halves(values):
    high = values.astype(BF16)
    return (high, (values - high.astype(F32)).astype(BF16))


def pick_wide(hot, values):
    high, low = halves(values)
    return matmul(hot, high) + matmul(hot, low)


def spread(hot, values):
    high, low = halves(values)
    return outer(hot, high) + outer(hot, low)


def hot_rows(indices, width):
    columns = lax.broadcasted_iota(jnp.int32, (indices.shape[0], width), 1)
    return jnp.where(columns == indices, 1.0, 0.0).astype(BF16)


def hidden_and_slope(preact):
    sigma = 1.0 / (1.0 + jnp.exp(-preact))
    return ((preact * sigma).astype(BF16), sigma * (1.0 + preact * (1.0 - sigma)))


def fused_kernel(
    sizes,
    grid_ref,
    mesh_ref,
    wg_ref,
    wm_ref,
    we_ref,
    ws_ref,
    wd_ref,
    wp_ref,
    index_ref,
    cot_ref,
    out_ref,
    ggrid_ref,
    gmesh_ref,
    terms_ref,
    weights,
    mesh_buf,
    cot_buf,
    slot_out,
    slot_in,
    halo_out,
    halo_in,
    halo_bout,
    halo_bin,
    slot_bout,
    slot_bin,
    sum_buf,
    share_out,
    share_in,
    term,
    pair_in,
    cross_out,
    cross_in,
    ring_out,
    ring_in,
    total_buf,
    gather_sems,
    dom_sems,
    sum_sems,
    share_sems,
    pair_sems,
    cross_sems,
):
    dom, feat, own, part, edges = sizes
    me = lax.axis_index("dom")
    f = lax.axis_index("feat")
    f1 = f + 1 - 2 * lax.rem(f, 2)
    f2 = lax.rem(f + 2, feat)
    f3 = lax.rem(f1 + 2, feat)

    def send(src, dst, sems, slot, **where):
        copy = pltpu.make_async_remote_copy(
            src_ref=src,
            dst_ref=dst,
            send_sem=sems.at[(0,) + slot],
            recv_sem=sems.at[(1,) + slot],
            device_id=where,
            device_id_type=MESH_ID,
        )
        copy.start()
        return copy

    def finish(copies):
        for copy in copies:
            copy.wait()

    def dom_exchange(kind, src, dst):
        copies = []
        for step in range(1, dom):
            peer = lax.rem(me + step, dom)
            copies.append(send(src.at[peer], dst.at[me], dom_sems, (kind, step), dom=peer))
        dst[me] = src[me]
        return copies

    def put_slabs(ref, rows):
        for index in range(dom):
            ref[index] = rows[index * SLAB : (index + 1) * SLAB].astype(BF16)

    def get_slabs(ref):
        return jnp.concatenate([ref[index].astype(F32) for index in range(dom)], axis=0).astype(BF16)

    def all_parts(ref):
        return jnp.concatenate([ref[index].astype(F32) for index in range(feat)], axis=0)

    barrier = pltpu.get_barrier_semaphore()
    for step in range(1, dom):
        pl.semaphore_signal(
            barrier, inc=1, device_id={"dom": lax.rem(me + step, dom)}, device_id_type=MESH_ID
        )
    for step in range(1, feat):
        pl.semaphore_signal(
            barrier, inc=1, device_id={"feat": lax.rem(f + step, feat)}, device_id_type=MESH_ID
        )
    mesh_buf[f] = mesh_ref[...]
    cot_buf[f] = cot_ref[...]
    slots = dom * SLAB
    send_hot = hot_rows(index_ref[0:slots], grid_ref.shape[0])
    put_slabs(slot_out, matmul(send_hot, grid_ref[...]))
    pl.semaphore_wait(barrier, dom + feat - 2)

    slot_copies = dom_exchange(0, slot_out, slot_in)
    refs = (wg_ref, wm_ref, we_ref, ws_ref, wd_ref, wp_ref)
    half = wg_ref.shape[0] // 2
    beyond = me + 1 - 2 * lax.rem(me, 2)
    mine = pl.ds(pl.multiple_of(lax.rem(me, 2) * half, half), half)
    theirs = pl.ds(pl.multiple_of((1 - lax.rem(me, 2)) * half, half), half)
    across, beside, passed, sideways, closing = {}, {}, {}, {}, {}

    def start_small(slot, buf):
        across[slot] = send(buf.at[f], buf.at[f], gather_sems, (0, slot), feat=f2)
        beside[slot] = send(buf.at[f], buf.at[f], gather_sems, (1, slot), feat=f1)

    def start_weight(slot):
        src, dst = refs[slot], weights.at[slot, f]
        across[slot] = send(src.at[mine], dst.at[mine], gather_sems, (0, slot), feat=f2)
        beside[slot] = send(src, dst, gather_sems, (1, slot), feat=f1)

    def relay_small(slot, buf):
        across[slot].wait_recv()
        passed[slot] = send(buf.at[f2], buf.at[f2], gather_sems, (2, slot), feat=f1)

    def relay(slot):
        across[slot].wait_recv()
        part_ref = weights.at[slot, f2, mine]
        sideways[slot] = send(part_ref, part_ref, gather_sems, (3, slot), dom=beyond)
        passed[slot] = send(part_ref, part_ref, gather_sems, (2, slot), feat=f1)

    def close(slot):
        sideways[slot].wait_recv()
        part_ref = weights.at[slot, f2, theirs]
        closing[slot] = send(part_ref, part_ref, gather_sems, (4, slot), feat=f1)

    start_weight(0)
    start_small(6, mesh_buf)
    for slot in (1, 2, 3, 4, 5):
        start_weight(slot)
    start_small(7, cot_buf)
    for slot, src in enumerate(refs):
        weights[slot, f] = src[...]
    relay(0)
    relay_small(6, mesh_buf)
    relay(1)
    relay(2)
    close(0)
    relay(3)
    close(1)
    relay(4)
    close(2)
    relay(5)
    relay_small(7, cot_buf)

    def whole(slot):
        return weights[slot].reshape(feat * weights.shape[2], weights.shape[3])

    def arrived(slot):
        beside[slot].wait_recv()
        passed[slot].wait_recv()
        if slot in closing:
            closing[slot].wait_recv()

    target_hot = hot_rows(index_ref[slots : 2 * slots], part)
    finish(slot_copies)
    grid_rows = get_slabs(slot_in)
    for slot in (0, 6, 1, 2):
        arrived(slot)
    mesh_part = all_parts(mesh_buf)
    mesh_rows = pick(target_hot, mesh_part.astype(BF16))
    preact_e = pick(grid_rows, whole(0)).astype(F32) + matmul(mesh_rows, whole(1))
    hidden_e, slope_e = hidden_and_slope(preact_e)
    normed_e, scaling_e = layer_norm(matmul(hidden_e, whole(2)))

    def feat_sum(kind, value):
        first = value.astype(BF16)
        sum_buf[kind, 0] = first
        copy = send(sum_buf.at[kind, 0], sum_buf.at[kind, 1], sum_sems, (kind, 0), feat=f1)
        yield
        copy.wait()
        both = (first.astype(F32) + sum_buf[kind, 1].astype(F32)).astype(BF16)
        sum_buf[kind, 2] = both
        copy = send(sum_buf.at[kind, 2], sum_buf.at[kind, 3], sum_sems, (kind, 1), feat=f2)
        yield
        copy.wait()
        yield both.astype(F32) + sum_buf[kind, 3].astype(F32)

    stages = feat_sum(0, spread(target_hot, normed_e))
    next(stages)
    next(stages)
    for slot in (3, 4, 5):
        close(slot)
    halo_hot = hot_rows(index_ref[2 * slots : 3 * slots], part)
    source_hot = hot_rows(index_ref[3 * slots : 3 * slots + edges], part + slots)
    edge_hot = hot_rows(index_ref[3 * slots + edges : 3 * slots + 2 * edges], part)
    latent = (mesh_part + next(stages)).astype(BF16)

    put_slabs(halo_out, matmul(halo_hot, latent))
    halo_copies = dom_exchange(1, halo_out, halo_in)
    dst_rows = pick(edge_hot, latent)
    for slot in (3, 4, 5, 7):
        arrived(slot)
    pre_dst = matmul(dst_rows, whole(4))
    upstream_p = matmul(edge_hot, all_parts(cot_buf).astype(BF16))
    finish(halo_copies)
    lookup = jnp.concatenate([latent, get_slabs(halo_in)], axis=0)
    src_rows = pick(source_hot, lookup)
    preact_p = matmul(src_rows, whole(3)) + pre_dst
    hidden_p, slope_p = hidden_and_slope(preact_p)
    normed_p, scaling_p = layer_norm(matmul(hidden_p, whole(5)))

    mid_p = norm_back(normed_p, scaling_p, upstream_p).astype(BF16)
    grad_p = (matmul_t(mid_p, whole(5)) * slope_p).astype(BF16)
    g_lookup = spread(source_hot, matmul_t(grad_p, whole(3)))
    put_slabs(halo_bout, g_lookup[part:])
    back_copies = dom_exchange(2, halo_bout, halo_bin)
    g_local = g_lookup[:part] + spread(edge_hot, matmul_t(grad_p, whole(4)))

    def scatter_own(kind, value):
        for index in range(feat):
            share_out[kind, index] = value[index * own : (index + 1) * own].astype(BF16)
        copies = []
        for step in range(1, feat):
            peer = lax.rem(f + step, feat)
            copies.append(
                send(
                    share_out.at[kind, peer],
                    share_in.at[kind, f],
                    share_sems,
                    (kind, step),
                    feat=peer,
                )
            )
        share_in[kind, f] = share_out[kind, f]
        return copies

    def own_sum(kind):
        total = share_in[kind, 0].astype(F32)
        for index in range(1, feat):
            total = total + share_in[kind, index].astype(F32)
        return total

    rows = term.shape[2]
    chunk = ring_out.shape[2]

    def start_terms(group, left, right):
        product = outer(left, right).astype(BF16)
        for shard in range(feat):
            term[group, shard] = product[shard * rows : (shard + 1) * rows]
        return [
            send(term.at[group, f3], pair_in.at[group, 1], pair_sems, (group, 1), feat=f1),
            send(term.at[group, f1], pair_in.at[group, 0], pair_sems, (group, 0), feat=f1),
        ]

    def cross_terms(group, copies):
        finish(copies)
        cross_out[group] = (
            term[group, f2].astype(F32) + pair_in[group, 1].astype(F32)
        ).astype(BF16)
        return [send(cross_out.at[group], cross_in.at[group], cross_sems, (group,), feat=f2)]

    def ring_terms(group, copies):
        finish(copies)
        share = (
            term[group, f].astype(F32)
            + pair_in[group, 0].astype(F32)
            + cross_in[group].astype(F32)
        ).astype(BF16)
        for piece in range(dom):
            ring_out[group, piece] = share[piece * chunk : (piece + 1) * chunk]
        return dom_exchange(4 + 2 * group, ring_out.at[group], ring_in.at[group])

    def total_terms(group, copies):
        finish(copies)
        total = ring_in[group, 0].astype(F32)
        for piece in range(1, dom):
            total = total + ring_in[group, piece].astype(F32)
        total_buf[group, me] = total.astype(BF16)
        copies = []
        for step in range(1, dom):
            peer = lax.rem(me + step, dom)
            copies.append(
                send(
                    total_buf.at[group, me],
                    total_buf.at[group, me],
                    dom_sems,
                    (5 + 2 * group, step),
                    dom=peer,
                )
            )
        return copies

    def write_terms(group, copies):
        finish(copies)
        for piece in range(dom):
            terms_ref[group, piece * chunk : (piece + 1) * chunk] = total_buf[group, piece]

    pairs = {
        3: start_terms(3, src_rows, grad_p),
        4: start_terms(4, dst_rows, grad_p),
        5: start_terms(5, hidden_p, mid_p),
    }
    finish(back_copies)
    g_local = g_local + outer(halo_hot, get_slabs(halo_bin))
    stages = feat_sum(1, g_local)
    next(stages)
    next(stages)
    proc_share = scatter_own(0, spread(edge_hot, normed_p))
    crossing = {group: cross_terms(group, pairs[group]) for group in (3, 4, 5)}
    cot_part = all_parts(cot_buf)
    node_grad = next(stages) + cot_part

    mid_e = norm_back(normed_e, scaling_e, pick_wide(target_hot, node_grad)).astype(BF16)
    pairs[2] = start_terms(2, hidden_e, mid_e)
    grad_e = (matmul_t(mid_e, whole(2)) * slope_e).astype(BF16)
    put_slabs(slot_bout, grad_e.astype(F32))
    slot_copies = dom_exchange(3, slot_bout, slot_bin)
    pairs[1] = start_terms(1, mesh_rows, grad_e)
    pairs[0] = start_terms(0, grid_rows, grad_e)
    crossing[2] = cross_terms(2, pairs[2])
    crossing[1] = cross_terms(1, pairs[1])
    crossing[0] = cross_terms(0, pairs[0])
    enc_share = scatter_own(1, spread(target_hot, matmul_t(grad_e, whole(1))))
    order = (3, 4, 5, 2, 1, 0)
    rings = {group: ring_terms(group, crossing[group]) for group in (3, 4, 5)}
    own_hot = hot_rows(f * own + lax.broadcasted_iota(jnp.int32, (own, 1), 0), part)
    own_grad = pick_wide(own_hot, node_grad)
    own_latent = matmul(own_hot, latent)
    finish(slot_copies)
    slot_rows = outer(send_hot, get_slabs(slot_bin)).astype(BF16)
    ggrid_ref[...] = matmul_t(slot_rows, whole(0)).astype(BF16)
    totals = {}
    totals[3] = total_terms(3, rings[3])
    rings[2] = ring_terms(2, crossing[2])
    totals[4] = total_terms(4, rings[4])
    rings[1] = ring_terms(1, crossing[1])
    totals[5] = total_terms(5, rings[5])
    rings[0] = ring_terms(0, crossing[0])
    finish(proc_share)
    out_ref[...] = (own_latent + own_sum(0)).astype(BF16)
    finish(enc_share)
    gmesh_ref[...] = (own_grad + own_sum(1)).astype(BF16)
    for group in (2, 1, 0):
        totals[group] = total_terms(group, rings[group])
    for group in order:
        write_terms(group, totals[group])
    for copies in (across, beside, passed, sideways, closing):
        for copy in copies.values():
            copy.wait_send()


def fused(
    grid_feat,
    mesh_feat,
    w_grid,
    w_mesh,
    w_enc2,
    w_src,
    w_dst,
    w_proc2,
    enc_send,
    enc_dst,
    hal_send,
    proc_src,
    proc_dst,
    cotangent,
):
    dom = lax.axis_size("dom")
    feat = lax.axis_size("feat")
    own, width = mesh_feat.shape
    part = own * feat
    edges = proc_src.shape[0]
    halo = hal_send.shape[1]
    shard = w_grid.shape[0]
    chunk = shard // dom

    def slabs(table):
        return jnp.pad(table, ((0, 0), (0, SLAB - table.shape[1])), constant_values=-1).reshape(-1)

    far = proc_src - part
    moved = jnp.where(far < 0, proc_src, part + far // halo * SLAB + far % halo)
    indices = jnp.concatenate([slabs(enc_send), slabs(enc_dst), slabs(hal_send), moved, proc_dst])
    slab = pltpu.VMEM((dom, SLAB, width), BF16)
    vmem = pl.BlockSpec(memory_space=pltpu.VMEM)
    factor = 1.0 / math.sqrt(own * dom * feat)
    out, g_grid, g_mesh, totals = pl.pallas_call(
        functools.partial(fused_kernel, (dom, feat, own, part, edges)),
        out_shape=(
            jax.ShapeDtypeStruct((own, width), BF16),
            jax.ShapeDtypeStruct(grid_feat.shape, BF16),
            jax.ShapeDtypeStruct((own, width), BF16),
        )
        + (jax.ShapeDtypeStruct((6, shard, width), BF16),),
        in_specs=[vmem] * 10,
        out_specs=(vmem,) * 4,
        scratch_shapes=[
            pltpu.VMEM((6, feat, shard, width), BF16),
            pltpu.VMEM((feat, own, width), BF16),
            pltpu.VMEM((feat, own, width), BF16),
            slab,
            slab,
            slab,
            slab,
            slab,
            slab,
            slab,
            slab,
            pltpu.VMEM((2, 4, part, width), BF16),
            pltpu.VMEM((2, feat, own, width), BF16),
            pltpu.VMEM((2, feat, own, width), BF16),
            pltpu.VMEM((6, feat, shard, width), BF16),
            pltpu.VMEM((6, 2, shard, width), BF16),
            pltpu.VMEM((6, shard, width), BF16),
            pltpu.VMEM((6, shard, width), BF16),
            pltpu.VMEM((6, dom, chunk, width), BF16),
            pltpu.VMEM((6, dom, chunk, width), BF16),
            pltpu.VMEM((6, dom, chunk, width), BF16),
            pltpu.SemaphoreType.DMA((2, 5, 8)),
            pltpu.SemaphoreType.DMA((2, 16, dom)),
            pltpu.SemaphoreType.DMA((2, 2, 2)),
            pltpu.SemaphoreType.DMA((2, 2, feat)),
            pltpu.SemaphoreType.DMA((2, 6, 2)),
            pltpu.SemaphoreType.DMA((2, 6)),
        ],
        compiler_params=pltpu.CompilerParams(
            collective_id=0, has_side_effects=True, vmem_limit_bytes=56 * 1024 * 1024
        ),
        name="fused_layer",
    )(
        grid_feat,
        mesh_feat,
        w_grid,
        w_mesh,
        w_enc2,
        w_src,
        w_dst,
        w_proc2,
        indices[:, None],
        cotangent,
    )
    return (out, g_grid, g_mesh) + tuple(factor * totals[index].astype(F32) for index in range(6))


def choose(*args):
    dom = lax.axis_size("dom")
    feat = lax.axis_size("feat")
    shard = args[2].shape[0]
    fits = max(args[8].shape[1], args[10].shape[1]) <= SLAB
    if feat == 4 and dom % 2 == 0 and shard % (dom * TILE) == 0 and fits:
        return fused(*args)
    return per_device(*args)


def solution(mesh):
    return jax.shard_map(
        choose,
        mesh=mesh,
        in_specs=(
            P(("dom", "feat"), None),
            P(("dom", "feat"), None),
            P("feat", None),
            P("feat", None),
            P("feat", None),
            P("feat", None),
            P("feat", None),
            P("feat", None),
            P(("dom", "feat"), None),
            P(("dom", "feat"), None),
            P("dom", None),
            P(("dom", "feat")),
            P(("dom", "feat")),
            P(("dom", "feat"), None),
        ),
        out_specs=(
            P(("dom", "feat"), None),
            P(("dom", "feat"), None),
            P(("dom", "feat"), None),
            P("feat", None),
            P("feat", None),
            P("feat", None),
            P("feat", None),
            P("feat", None),
            P("feat", None),
        ),
        check_vma=False,
    )
```
